32 devices in a mesh: gx: 8 (over y, x, core), gy: 4 (over z).
Axes of the slice: x: 2, y: 2, z: 4, core: 2. Of those that a mesh axis runs over, the one named last changes fastest.
Arguments:
- right_side: float32 [32, 256, 256], P('gx', 'gy'), may hold values from -40 to 40
- kappa_sq: float32 [32, 256, 256], P('gx', 'gy'), may hold values from 0.5 to 4
Outputs:
- solution_field: float32 [32, 256, 256], P('gx', 'gy')
- residual: float32 [32, 256, 256], P('gx', 'gy')
- residual_rms: float32 [3], replicated
The draws below stay inside these ranges and needn't reach their ends.
All inputs are finite; a program needn't handle non-finite values.
Results may differ from the reference program's by a relative error of at most 0.00016.
Values sent between devices are 32-bit elements; how exact they have to be, the bound alone decides.
A program may use at most 64 MiB of HBM per device.

```python
import math
import jax
import jax.numpy as jnp

CZ = 256
ITERS = 3
NX = 32
NY = 256


def draw_right_side(key, part):
    first = jax.random.fold_in(key, 11)
    noise = jax.random.normal(first, (NX, NY, CZ), jnp.float32)
    place = jnp.arange(NX, dtype=jnp.float32) / NX
    rising = 1.0 + 2.0 * place
    values = noise * rising[:, None, None]
    return jnp.clip(values, -40.0, 40.0).astype(jnp.float32)


def level_of(key, shape, shards, least, largest):
    loudness = 1.0
    for axis_at, parts in shards:
        heights = jax.random.uniform(jax.random.fold_in(jax.random.fold_in(key, 6), axis_at), (parts,), jnp.float32, least / len(shards), largest / len(shards))
        loudness = loudness * jnp.repeat(jnp.exp(heights), shape[axis_at] // parts).reshape((-1,) + (1,) * (len(shape) - 1 - axis_at))
    return loudness


def setup_inputs(seed: int = 0) -> dict:
    key_of = jax.random.split(jax.random.key(seed), 3)
    return {
        "right_side": draw_right_side(jax.random.fold_in(key_of[2], 71), 0),
        "kappa_sq": jnp.clip(jnp.exp(math.log(4.0) - 2.0794415 * jax.random.uniform(key_of[1], (NX, NY, CZ), jnp.float32) ** level_of(key_of[1], (NX, NY, CZ), ((0, 8), (1, 4)), -0.2, 0.2)), 0.5, 4.0),
    }


def kpass(field, kappa_sq):
    beside = jnp.roll(field, 1, 0) + jnp.roll(field, -1, 0)
    beside = beside + jnp.roll(field, 1, 1) + jnp.roll(field, -1, 1)
    beside = beside + jnp.roll(field, 1, 2) + jnp.roll(field, -1, 2)
    return (6.0 + kappa_sq) * field - beside

def operate(field, kappa_sq):
    return kpass(kpass(field, kappa_sq), kappa_sq)

def reference(right_side, kappa_sq):
    shifted = 6.0 + kappa_sq
    precond = 1.0 / (shifted * shifted + 6.0)
    cells = right_side.shape[0] * right_side.shape[1] * right_side.shape[2]
    solution_field = jnp.zeros_like(right_side)
    residual = right_side
    u_vec = precond * residual
    w_vec = operate(u_vec, kappa_sq)
    p_vec = jnp.zeros_like(right_side)
    s_vec = jnp.zeros_like(right_side)
    q_vec = jnp.zeros_like(right_side)
    z_vec = jnp.zeros_like(right_side)
    norms = []
    gamma_old = jnp.float32(1.0)
    alpha_old = jnp.float32(1.0)
    for step in range(ITERS):
        gamma = jnp.sum(residual * u_vec)
        delta = jnp.sum(w_vec * u_vec)
        norm_sq = jnp.sum(residual * residual)
        norms.append(jnp.sqrt(norm_sq / cells))
        m_vec = precond * w_vec
        n_vec = operate(m_vec, kappa_sq)
        if step == 0:
            beta = jnp.float32(0.0)
            alpha = gamma / delta
        else:
            beta = gamma / gamma_old
            alpha = gamma / (delta - beta * gamma / alpha_old)
        z_vec = n_vec + beta * z_vec
        q_vec = m_vec + beta * q_vec
        s_vec = w_vec + beta * s_vec
        p_vec = u_vec + beta * p_vec
        solution_field = solution_field + alpha * p_vec
        residual = residual - alpha * s_vec
        u_vec = u_vec - alpha * q_vec
        w_vec = w_vec - alpha * z_vec
        gamma_old = gamma
        alpha_old = alpha
    return (solution_field, residual, jnp.stack(norms).astype(jnp.float32))
```

```python
import functools
import jax
import jax.numpy as jnp
from jax import lax
from jax.experimental import pallas as pl
from jax.experimental.pallas import tpu as pltpu
from jax.sharding import PartitionSpec as P

ITERS = 3
MESH = pl.DeviceIdType.MESH


def shifted(c):
    return [None] + c[:-1]


def plus(a, b, scale):
    out = []
    for one, two in zip(a, b):
        two = None if two is None else two * scale
        out.append(one if two is None else two if one is None else one + two)
    return out


def form(c, entry):
    total = None
    for i, one in enumerate(c):
        for j, two in enumerate(c):
            if one is not None and two is not None and i < ITERS and j < ITERS:
                term = one * two * entry(i, j)
                total = term if total is None else total + term
    return total


def coefficients(mu, dots, cells):
    one = jnp.ones_like(mu[0])
    res = [one] + [None] * ITERS
    step = [None] * (ITERS + 1)
    sol = [None] * (ITERS + 1)
    norms = []
    for i in range(ITERS):
        gamma = form(res, lambda a, b: mu[a + b])
        delta = form(res, lambda a, b: mu[a + b + 1])
        norms.append(jnp.sqrt(form(res, lambda a, b: dots[min(a, b), max(a, b)]) / cells))
        if i == 0:
            alpha = gamma / delta
            step = list(res)
        else:
            beta = gamma / gamma_old
            alpha = gamma / (delta - beta * gamma / alpha_old)
            step = plus(res, step, beta)
        sol = plus(sol, step, alpha)
        res = plus(res, shifted(step), -alpha)
        gamma_old, alpha_old = gamma, alpha
    return sol, res, norms


def kernel(
    nx, ny, cells, rhs_hbm, kappa_hbm, sol_ref, res_ref, norms_ref,
    v_ref, y_ref, t_ref, d_ref, m_ref, face_ref, edge_out, edge_in, corner_out, corner_in,
    slots, load_sem, face_send, face_recv, edge_send, edge_recv, corner_send, corner_recv,
    sum_send, sum_recv,
):
    layers, rows, cols = rhs_hbm.shape
    ix, iy = lax.axis_index("gx"), lax.axis_index("gy")
    count = nx * ny
    me = ix * ny + iy
    load_k = pltpu.make_async_copy(kappa_hbm, d_ref, load_sem.at[0])
    load_r = pltpu.make_async_copy(rhs_hbm, v_ref.at[0], load_sem.at[1])
    load_k.start()
    load_r.start()

    barrier = pltpu.get_barrier_semaphore()

    def greet(k, carry):
        other = lax.rem(me + k, count)
        pl.semaphore_signal(
            barrier, inc=1, device_id=(other // ny, lax.rem(other, ny)), device_id_type=MESH
        )
        return carry

    lax.fori_loop(1, count, greet, 0)

    x_of = (lax.rem(ix + nx - 1, nx), lax.rem(ix + 1, nx))
    y_of = (lax.rem(iy + ny - 1, ny), lax.rem(iy + 1, ny))
    row = lax.broadcasted_iota(jnp.int32, (rows, cols), 0)
    first, last = row == 0, row == rows - 1

    def lateral(x):
        up = jnp.where(first, 0.0, pltpu.roll(x, 1, 0))
        down = jnp.where(last, 0.0, pltpu.roll(x, rows - 1, 0))
        return (pltpu.roll(x, 1, 1) + pltpu.roll(x, cols - 1, 1)) + (up + down)

    def local_k(get, l):
        x = get(l)
        out = d_ref[l] * x - lateral(x)
        if l > 0:
            out = out - get(l - 1)
        if l < layers - 1:
            out = out - get(l + 1)
        return out

    def tile_sum(x):
        return jnp.sum(x, axis=(0, 1), keepdims=True)

    load_k.wait()
    for l in range(layers):
        d = 6.0 + d_ref[l]
        d_ref[l] = d
        m_ref[l] = 1.0 / (d * d + 6.0)
    load_r.wait()

    ends = (0, layers - 1)
    mu, dots = ([], {})
    for j in range(ITERS):
        order = [0, layers - 1] + list(range(1, layers - 1)) if layers > 1 else [0]
        for l in order:
            y_ref[j, l] = m_ref[l] * v_ref[j, l]
        for side in range(2):
            at = (0, rows - 1)[side]
            for k in range(2):
                corner_out[j, 2 * k + side] = y_ref[j, ends[k], pl.ds(at, 1), :]
        if j == 0:
            pl.semaphore_wait(barrier, count - 1)
        copies = []
        for k in range(2):
            copies.append(
                pltpu.make_async_remote_copy(
                    src_ref=y_ref.at[j, ends[k]],
                    dst_ref=face_ref.at[j, 1 - k, 0],
                    send_sem=face_send.at[j, 1 - k, 0],
                    recv_sem=face_recv.at[j, 1 - k, 0],
                    device_id=(x_of[k], iy),
                    device_id_type=MESH,
                )
            )
        for k in range(2):
            for side in range(2):
                copies.append(
                    pltpu.make_async_remote_copy(
                        src_ref=corner_out.at[j, 2 * k + side],
                        dst_ref=corner_in.at[j, 2 * (1 - k) + 1 - side],
                        send_sem=corner_send.at[j, 2 * (1 - k) + 1 - side],
                        recv_sem=corner_recv.at[j, 2 * (1 - k) + 1 - side],
                        device_id=(x_of[k], y_of[side]),
                        device_id_type=MESH,
                    )
                )
        for copy in copies:
            copy.start()
        get_y = lambda l: y_ref[j, l]
        for l in order:
            t_ref[j, l] = local_k(get_y, l)
        for side in range(2):
            at = (0, rows - 1)[side]
            for l in range(layers):
                edge_out[j, side, pl.ds(l, 1), :] = y_ref[j, l, pl.ds(at, 1), :]
                edge_out[j, side, pl.ds(layers + l, 1), :] = t_ref[j, l, pl.ds(at, 1), :]
        later = []
        for side in range(2):
            later.append(
                pltpu.make_async_remote_copy(
                    src_ref=edge_out.at[j, side],
                    dst_ref=edge_in.at[j, 1 - side],
                    send_sem=edge_send.at[j, 1 - side],
                    recv_sem=edge_recv.at[j, 1 - side],
                    device_id=(ix, y_of[side]),
                    device_id_type=MESH,
                )
            )
        for k in range(2):
            later.append(
                pltpu.make_async_remote_copy(
                    src_ref=t_ref.at[j, ends[k]],
                    dst_ref=face_ref.at[j, 1 - k, 1],
                    send_sem=face_send.at[j, 1 - k, 1],
                    recv_sem=face_recv.at[j, 1 - k, 1],
                    device_id=(x_of[k], iy),
                    device_id_type=MESH,
                )
            )
        for copy in later:
            copy.start()
        copies = copies + later
        mu.append(tile_sum(sum(v_ref[j, l] * y_ref[j, l] for l in range(layers))))
        for i in range(j + 1):
            dots[i, j] = tile_sum(sum(v_ref[i, l] * v_ref[j, l] for l in range(layers)))
        for copy in copies:
            copy.wait()
        full = ITERS + j % 2
        for k in range(2):
            face_ref[j, k, 1] = face_ref[j, k, 1] - y_ref[j, ends[k]]
        for l in range(layers):
            t = t_ref[j, l]
            if l == 0:
                t = t - face_ref[j, 0, 0]
            if l == layers - 1:
                t = t - face_ref[j, 1, 0]
            t_ref[full, l] = t
            for side in range(2):
                at = pl.ds((0, rows - 1)[side], 1)
                t_ref[full, l, at, :] = t_ref[full, l, at, :] - edge_in[j, side, pl.ds(l, 1), :]
        mu.append(tile_sum(sum(t_ref[full, l] * t_ref[full, l] for l in range(layers))))
        if j == ITERS - 1:
            start_sums(mu, dots, slots, sum_send, sum_recv, me, count, ny)
        get_t = lambda l: t_ref[full, l]
        for l in range(layers):
            v = local_k(get_t, l)
            if l == 0:
                v = v - face_ref[j, 0, 1]
            if l == layers - 1:
                v = v - face_ref[j, 1, 1]
            v_ref[j + 1, l] = v
            for side in range(2):
                at = pl.ds((0, rows - 1)[side], 1)
                line = v_ref[j + 1, l, at, :] + y_ref[j, l, at, :]
                line = line - edge_in[j, side, pl.ds(layers + l, 1), :]
                for k in range(2):
                    if l == ends[k]:
                        line = line + 2.0 * corner_in[j, 2 * k + side]
                v_ref[j + 1, l, at, :] = line

    all_slots = slots.at[pl.ds(0, count - 1)]
    pltpu.make_async_copy(all_slots, all_slots, sum_send).wait()
    pltpu.make_async_copy(all_slots, all_slots, sum_recv).wait()
    total = jnp.sum(slots[...], axis=0)
    names = [("mu", i) for i in range(2 * ITERS)] + sorted(dots)
    got = {name: total[:, k : k + 1] for k, name in enumerate(names)}
    mu = [got["mu", i] for i in range(2 * ITERS)]
    sol, res, norms = coefficients(mu, got, float(cells))
    for i in range(ITERS):
        norms_ref[i] = norms[i][0, 0]
    for l in range(layers):
        x = sol[0] * y_ref[0, l]
        r = v_ref[0, l]
        for i in range(1, ITERS):
            x = x + sol[i] * y_ref[i, l]
        for i in range(1, ITERS + 1):
            r = r + res[i] * v_ref[i, l]
        sol_ref[l] = x
        res_ref[l] = r


def start_sums(mu, dots, slots, sum_send, sum_recv, me, count, ny):
    lane = lax.broadcasted_iota(jnp.int32, (1, slots.shape[-1]), 1)
    line = jnp.zeros(lane.shape, jnp.float32)
    for k, value in enumerate(mu + [dots[name] for name in sorted(dots)]):
        line = jnp.where(lane == k, value, line)
    slots[me] = line

    def send(k, carry):
        other = lax.rem(me + k, count)
        pltpu.make_async_remote_copy(
            src_ref=slots.at[me],
            dst_ref=slots.at[me],
            send_sem=sum_send,
            recv_sem=sum_recv,
            device_id=(other // ny, lax.rem(other, ny)),
            device_id_type=MESH,
        ).start()
        return carry

    lax.fori_loop(1, count, send, 0)


def body(right_side, kappa_sq):
    nx, ny = lax.axis_size("gx"), lax.axis_size("gy")
    shape = right_side.shape
    layers, rows, cols = shape
    cells = nx * layers * ny * rows * cols
    f32 = jnp.float32
    dma = pltpu.SemaphoreType.DMA
    vmem = pl.BlockSpec(memory_space=pltpu.VMEM)
    return pl.pallas_call(
        functools.partial(kernel, nx, ny, cells),
        out_shape=(
            jax.ShapeDtypeStruct(shape, f32),
            jax.ShapeDtypeStruct(shape, f32),
            jax.ShapeDtypeStruct((ITERS,), f32),
        ),
        in_specs=[pl.BlockSpec(memory_space=pl.ANY)] * 2,
        out_specs=(vmem, vmem, pl.BlockSpec(memory_space=pltpu.SMEM)),
        scratch_shapes=[
            pltpu.VMEM((ITERS + 1,) + shape, f32),
            pltpu.VMEM((ITERS,) + shape, f32),
            pltpu.VMEM((ITERS + 2,) + shape, f32),
            pltpu.VMEM(shape, f32),
            pltpu.VMEM(shape, f32),
            pltpu.VMEM((ITERS, 2, 2, rows, cols), f32),
            pltpu.VMEM((ITERS, 2, 2 * layers, cols), f32),
            pltpu.VMEM((ITERS, 2, 2 * layers, cols), f32),
            pltpu.VMEM((ITERS, 4, 1, cols), f32),
            pltpu.VMEM((ITERS, 4, 1, cols), f32),
            pltpu.VMEM((nx * ny, 1, 128), f32),
            dma((2,)),
            dma((ITERS, 2, 2)),
            dma((ITERS, 2, 2)),
            dma((ITERS, 2)),
            dma((ITERS, 2)),
            dma((ITERS, 4)),
            dma((ITERS, 4)),
            dma(()),
            dma(()),
        ],
        compiler_params=pltpu.CompilerParams(collective_id=0, has_side_effects=True),
    )(right_side, kappa_sq)


def solution(mesh):
    return jax.shard_map(
        body,
        mesh=mesh,
        in_specs=(P("gx", "gy", None), P("gx", "gy", None)),
        out_specs=(P("gx", "gy", None), P("gx", "gy", None), P()),
        check_vma=False,
    )
```

```python
import functools
import jax
import jax.numpy as jnp
from jax import lax
from jax.experimental import pallas as pl
from jax.experimental.pallas import tpu as pltpu
from jax.sharding import PartitionSpec as P

ITERS = 3
MESH = pl.DeviceIdType.MESH


def shifted(c):
    return [None] + c[:-1]


def plus(a, b, scale):
    out = []
    for one, two in zip(a, b):
        two = None if two is None else two * scale
        out.append(one if two is None else two if one is None else one + two)
    return out


def form(c, entry):
    total = None
    for i, one in enumerate(c):
        for j, two in enumerate(c):
            if one is not None and two is not None and i < ITERS and j < ITERS:
                term = one * two * entry(i, j)
                total = term if total is None else total + term
    return total


def coefficients(mu, dots, cells):
    one = jnp.ones_like(mu[0])
    res = [one] + [None] * ITERS
    step = [None] * (ITERS + 1)
    sol = [None] * (ITERS + 1)
    norms = []
    for i in range(ITERS):
        gamma = form(res, lambda a, b: mu[a + b])
        delta = form(res, lambda a, b: mu[a + b + 1])
        norms.append(jnp.sqrt(form(res, lambda a, b: dots[min(a, b), max(a, b)]) / cells))
        if i == 0:
            alpha = gamma / delta
            step = list(res)
        else:
            beta = gamma / gamma_old
            alpha = gamma / (delta - beta * gamma / alpha_old)
            step = plus(res, step, beta)
        sol = plus(sol, step, alpha)
        res = plus(res, shifted(step), -alpha)
        gamma_old, alpha_old = gamma, alpha
    return sol, res, norms


def kernel(
    nx, ny, cells, rhs_hbm, kappa_hbm, *refs,
):
    (
    v_ref, y_ref, coef_ref, t_ref, d_ref, m_ref, face_ref, edge_out, edge_in, corner_out, corner_in,
    slots, load_sem, face_send, face_recv, edge_send, edge_recv, corner_send, corner_recv,
    sum_send, sum_recv,
    ) = refs
    layers, rows, cols = rhs_hbm.shape
    ix, iy = lax.axis_index("gx"), lax.axis_index("gy")
    count = nx * ny
    me = ix * ny + iy
    load_k = pltpu.make_async_copy(kappa_hbm, d_ref, load_sem.at[0])
    load_r = pltpu.make_async_copy(rhs_hbm, v_ref.at[0], load_sem.at[1])
    load_k.start()
    load_r.start()

    barrier = pltpu.get_barrier_semaphore()

    def greet(k, carry):
        other = lax.rem(me + k, count)
        pl.semaphore_signal(
            barrier, inc=1, device_id=(other // ny, lax.rem(other, ny)), device_id_type=MESH
        )
        return carry

    lax.fori_loop(1, count, greet, 0)

    x_of = (lax.rem(ix + nx - 1, nx), lax.rem(ix + 1, nx))
    y_of = (lax.rem(iy + ny - 1, ny), lax.rem(iy + 1, ny))
    row = lax.broadcasted_iota(jnp.int32, (rows, cols), 0)
    first, last = row == 0, row == rows - 1

    def lateral(x):
        up = jnp.where(first, 0.0, pltpu.roll(x, 1, 0))
        down = jnp.where(last, 0.0, pltpu.roll(x, rows - 1, 0))
        return (pltpu.roll(x, 1, 1) + pltpu.roll(x, cols - 1, 1)) + (up + down)

    def local_k(get, l):
        x = get(l)
        out = d_ref[l] * x - lateral(x)
        if l > 0:
            out = out - get(l - 1)
        if l < layers - 1:
            out = out - get(l + 1)
        return out

    def tile_sum(x):
        return jnp.sum(x, axis=(0, 1), keepdims=True)

    load_k.wait()
    for l in range(layers):
        d = 6.0 + d_ref[l]
        d_ref[l] = d
        m_ref[l] = 1.0 / (d * d + 6.0)
    load_r.wait()

    ends = (0, layers - 1)
    mu, dots = ([], {})
    sends = []
    order = [0, layers - 1] + list(range(1, layers - 1)) if layers > 1 else [0]
    inner_first = list(range(1, layers - 1)) + [0, layers - 1] if layers > 1 else [0]

    def remote(src, dst, send, recv, device):
        copy = pltpu.make_async_remote_copy(
            src_ref=src, dst_ref=dst, send_sem=send, recv_sem=recv,
            device_id=device, device_id_type=MESH,
        )
        sends.append(copy)
        return copy

    for j in range(ITERS):
        for l in order:
            y_ref[j, l] = m_ref[l] * v_ref[j, l]
        for side in range(2):
            at = pl.ds((0, rows - 1)[side], 1)
            for k in range(2):
                corner_out[j, 2 * k + side] = y_ref[j, ends[k], at, :]
            for l in range(layers):
                edge_out[j, 0, side, pl.ds(l, 1), :] = y_ref[j, l, at, :]
        if j == 0:
            pl.semaphore_wait(barrier, count - 1)
        edges = [
            [
                remote(
                    edge_out.at[j, part, side], edge_in.at[j, part, 1 - side],
                    edge_send.at[j, part, side], edge_recv.at[j, part, 1 - side],
                    (ix, y_of[side]),
                )
                for side in range(2)
            ]
            for part in range(2)
        ]
        corners = [
            remote(
                corner_out.at[j, 2 * k + side], corner_in.at[j, 2 * (1 - k) + 1 - side],
                corner_send.at[j, 2 * k + side], corner_recv.at[j, 2 * (1 - k) + 1 - side],
                (x_of[k], y_of[side]),
            )
            for k in range(2)
            for side in range(2)
        ]
        faces = [
            [
                remote(
                    src.at[j, ends[k]], face_ref.at[j, 1 - k, part],
                    face_send.at[j, k, part], face_recv.at[j, 1 - k, part],
                    (x_of[k], iy),
                )
                for k in range(2)
            ]
            for part, src in enumerate((y_ref, t_ref))
        ]
        for copy in edges[0] + corners + faces[0]:
            copy.start()
        get_y = lambda l: y_ref[j, l]
        for l in order:
            t_ref[j, l] = local_k(get_y, l)
        for side in range(2):
            for l in range(layers):
                at = pl.ds((0, rows - 1)[side], 1)
                edge_out[j, 1, side, pl.ds(l, 1), :] = t_ref[j, l, at, :]
        for copy in edges[1] + faces[1]:
            copy.start()
        mu.append(tile_sum(sum(v_ref[j, l] * y_ref[j, l] for l in range(layers))))
        for i in range(j + 1):
            dots[i, j] = tile_sum(sum(v_ref[i, l] * v_ref[j, l] for l in range(layers)))
        for copy in faces[0] + edges[0]:
            copy.wait_recv()
        full = ITERS + j % 2
        for l in range(layers):
            t = t_ref[j, l]
            if l == 0:
                t = t - face_ref[j, 0, 0]
            if l == layers - 1:
                t = t - face_ref[j, 1, 0]
            t_ref[full, l] = t
            for side in range(2):
                at = pl.ds((0, rows - 1)[side], 1)
                t_ref[full, l, at, :] = t_ref[full, l, at, :] - edge_in[j, 0, side, pl.ds(l, 1), :]
        mu.append(tile_sum(sum(t_ref[full, l] * t_ref[full, l] for l in range(layers))))
        if j == ITERS - 1:
            start_sums(mu, dots, slots, sum_send, sum_recv, me, count, ny)
        get_t = lambda l: t_ref[full, l]
        for l in range(layers):
            v = local_k(get_t, l)
            for k in range(2):
                if l == ends[k]:
                    v = v + y_ref[j, l]
            v_ref[j + 1, l] = v
            for side in range(2):
                at = pl.ds((0, rows - 1)[side], 1)
                v_ref[j + 1, l, at, :] = v_ref[j + 1, l, at, :] + y_ref[j, l, at, :]
        for copy in edges[1] + corners:
            copy.wait_recv()
        for l in range(layers):
            for side in range(2):
                at = pl.ds((0, rows - 1)[side], 1)
                line = v_ref[j + 1, l, at, :] - edge_in[j, 1, side, pl.ds(l, 1), :]
                for k in range(2):
                    if l == ends[k]:
                        line = line + 2.0 * corner_in[j, 2 * k + side]
                v_ref[j + 1, l, at, :] = line
        for copy in faces[1]:
            copy.wait_recv()
        for k in range(2):
            v_ref[j + 1, ends[k]] = v_ref[j + 1, ends[k]] - face_ref[j, k, 1]

    for copy in sends:
        copy.wait_send()
    all_slots = slots.at[pl.ds(0, count - 1)]
    pltpu.make_async_copy(all_slots, all_slots, sum_send).wait()
    pltpu.make_async_copy(all_slots, all_slots, sum_recv).wait()
    total = jnp.sum(slots[...], axis=0)
    names = [("mu", i) for i in range(2 * ITERS)] + sorted(dots)
    got = {name: total[:, k : k + 1] for k, name in enumerate(names)}
    mu = [got["mu", i] for i in range(2 * ITERS)]
    sol, res, norms = coefficients(mu, got, float(cells))
    for k, value in enumerate(norms + sol[:ITERS] + res[1:]):
        coef_ref[k] = value[0, 0]


def start_sums(mu, dots, slots, sum_send, sum_recv, me, count, ny):
    lane = lax.broadcasted_iota(jnp.int32, (1, slots.shape[-1]), 1)
    line = jnp.zeros(lane.shape, jnp.float32)
    for k, value in enumerate(mu + [dots[name] for name in sorted(dots)]):
        line = jnp.where(lane == k, value, line)
    slots[me] = line

    def send(k, carry):
        other = lax.rem(me + k, count)
        pltpu.make_async_remote_copy(
            src_ref=slots.at[me],
            dst_ref=slots.at[me],
            send_sem=sum_send,
            recv_sem=sum_recv,
            device_id=(other // ny, lax.rem(other, ny)),
            device_id_type=MESH,
        ).start()
        return carry

    lax.fori_loop(1, count, send, 0)


def finish(coef, v_ref, y_ref, sol_ref, res_ref, norms_ref):
    for i in range(ITERS):
        norms_ref[i] = coef[i]
    for l in range(v_ref.shape[1]):
        sol = coef[ITERS] * y_ref[0, l]
        res = v_ref[0, l]
        for i in range(1, ITERS):
            sol = sol + coef[ITERS + i] * y_ref[i, l]
        for i in range(1, ITERS + 1):
            res = res + coef[2 * ITERS + i - 1] * v_ref[i, l]
        sol_ref[l] = sol
        res_ref[l] = res


def body(right_side, kappa_sq):
    nx, ny = lax.axis_size("gx"), lax.axis_size("gy")
    shape = right_side.shape
    layers, rows, cols = shape
    cells = nx * layers * ny * rows * cols
    f32 = jnp.float32
    dma = pltpu.SemaphoreType.DMA
    whole = pl.BlockSpec(memory_space=pltpu.VMEM)
    smem = pl.BlockSpec(memory_space=pltpu.SMEM)
    out = pl.pallas_call(
        functools.partial(kernel, nx, ny, cells),
        out_shape=(
            pltpu.VMEM((ITERS + 1,) + shape, f32),
            pltpu.VMEM((ITERS,) + shape, f32),
            pltpu.SMEM((3 * ITERS,), f32),
        ),
        in_specs=[pl.BlockSpec(memory_space=pl.ANY)] * 2,
        out_specs=(whole, whole, smem),
        scratch_shapes=[
            pltpu.VMEM((ITERS + 2,) + shape, f32),
            pltpu.VMEM(shape, f32),
            pltpu.VMEM(shape, f32),
            pltpu.VMEM((ITERS, 2, 2, rows, cols), f32),
            pltpu.VMEM((ITERS, 2, 2, layers, cols), f32),
            pltpu.VMEM((ITERS, 2, 2, layers, cols), f32),
            pltpu.VMEM((ITERS, 4, 1, cols), f32),
            pltpu.VMEM((ITERS, 4, 1, cols), f32),
            pltpu.VMEM((nx * ny, 1, 128), f32),
            dma((2,)),
            dma((ITERS, 2, 2)),
            dma((ITERS, 2, 2)),
            dma((ITERS, 2, 2)),
            dma((ITERS, 2, 2)),
            dma((ITERS, 4)),
            dma((ITERS, 4)),
            dma(()),
            dma(()),
        ],
        compiler_params=pltpu.CompilerParams(collective_id=0, has_side_effects=True),
    )(right_side, kappa_sq)
    return pl.pallas_call(
        finish,
        out_shape=(
            jax.ShapeDtypeStruct(shape, f32),
            jax.ShapeDtypeStruct(shape, f32),
            jax.ShapeDtypeStruct((ITERS,), f32),
        ),
        in_specs=[smem, whole, whole],
        out_specs=(whole, whole, smem),
    )(out[2], *(pltpu.with_memory_space_constraint(x, pltpu.VMEM) for x in out[:2]))


def solution(mesh):
    return jax.shard_map(
        body,
        mesh=mesh,
        in_specs=(P("gx", "gy", None), P("gx", "gy", None)),
        out_specs=(P("gx", "gy", None), P("gx", "gy", None), P()),
        check_vma=False,
    )
```

```python
import functools
import jax
import jax.numpy as jnp
from jax import lax
from jax.experimental import pallas as pl
from jax.experimental.pallas import tpu as pltpu
from jax.sharding import PartitionSpec as P

ITERS = 3
MESH = pl.DeviceIdType.MESH


def shifted(c):
    return [None] + c[:-1]


def plus(a, b, scale):
    out = []
    for one, two in zip(a, b):
        two = None if two is None else two * scale
        out.append(one if two is None else two if one is None else one + two)
    return out


def form(c, entry):
    total = None
    for i, one in enumerate(c):
        for j, two in enumerate(c):
            if one is not None and two is not None and i < ITERS and j < ITERS:
                term = one * two * entry(i, j)
                total = term if total is None else total + term
    return total


def coefficients(mu, dots, cells):
    one = jnp.ones_like(mu[0])
    res = [one] + [None] * ITERS
    step = [None] * (ITERS + 1)
    sol = [None] * (ITERS + 1)
    norms = []
    for i in range(ITERS):
        gamma = form(res, lambda a, b: mu[a + b])
        delta = form(res, lambda a, b: mu[a + b + 1])
        norms.append(jnp.sqrt(form(res, lambda a, b: dots[min(a, b), max(a, b)]) / cells))
        if i == 0:
            alpha = gamma / delta
            step = list(res)
        else:
            beta = gamma / gamma_old
            alpha = gamma / (delta - beta * gamma / alpha_old)
            step = plus(res, step, beta)
        sol = plus(sol, step, alpha)
        res = plus(res, shifted(step), -alpha)
        gamma_old, alpha_old = gamma, alpha
    return sol, res, norms


def kernel(
    nx, ny, cells, rhs_hbm, kappa_hbm, *refs,
):
    (
    v_ref, y_ref, coef_ref, t_ref, d_ref, m_ref, face_ref, edge_out, edge_in, corner_out, corner_in,
    slots, load_sem, face_send, face_recv, edge_send, edge_recv, corner_send, corner_recv,
    sum_send, sum_recv,
    ) = refs
    layers, rows, cols = rhs_hbm.shape
    ix, iy = lax.axis_index("gx"), lax.axis_index("gy")
    count = nx * ny
    me = ix * ny + iy
    load_k = pltpu.make_async_copy(kappa_hbm, d_ref, load_sem.at[0])
    load_r = pltpu.make_async_copy(rhs_hbm, v_ref.at[0], load_sem.at[1])
    load_k.start()
    load_r.start()

    barrier = pltpu.get_barrier_semaphore()

    near = ny // 2 <= ITERS

    def greet(x, y):
        pl.semaphore_signal(barrier, inc=1, device_id=(x, y), device_id_type=MESH)

    def greet_any(k, carry):
        other = lax.rem(me + k, count)
        greet(other // ny, lax.rem(other, ny))
        return carry

    def greet_x(k, carry):
        greet(lax.rem(ix + k, nx), iy)
        return carry

    def greet_y(k, carry):
        greet(ix, lax.rem(iy + k, ny))
        return carry

    if near:
        lax.fori_loop(1, ny, greet_y, 0)
        lax.fori_loop(1, nx, greet_x, 0)
        greetings = nx - 1 + ny - 1
    else:
        lax.fori_loop(1, count, greet_any, 0)
        greetings = count - 1

    x_of = (lax.rem(ix + nx - 1, nx), lax.rem(ix + 1, nx))
    y_of = (lax.rem(iy + ny - 1, ny), lax.rem(iy + 1, ny))
    row = lax.broadcasted_iota(jnp.int32, (rows, cols), 0)
    first, last = row == 0, row == rows - 1

    def lateral(x):
        up = jnp.where(first, 0.0, pltpu.roll(x, 1, 0))
        down = jnp.where(last, 0.0, pltpu.roll(x, rows - 1, 0))
        return (pltpu.roll(x, 1, 1) + pltpu.roll(x, cols - 1, 1)) + (up + down)

    def local_k(get, l):
        x = get(l)
        out = d_ref[l] * x - lateral(x)
        if l > 0:
            out = out - get(l - 1)
        if l < layers - 1:
            out = out - get(l + 1)
        return out

    def tile_sum(x):
        return jnp.sum(x, axis=(0, 1), keepdims=True)

    load_k.wait()
    for l in range(layers):
        d = 6.0 + d_ref[l]
        d_ref[l] = d
        m_ref[l] = 1.0 / (d * d + 6.0)
    load_r.wait()

    ends = (0, layers - 1)
    mu, dots = ([], {})
    sends = []
    order = [0, layers - 1] + list(range(1, layers - 1)) if layers > 1 else [0]
    inner_first = list(range(1, layers - 1)) + [0, layers - 1] if layers > 1 else [0]

    def remote(src, dst, send, recv, device):
        copy = pltpu.make_async_remote_copy(
            src_ref=src, dst_ref=dst, send_sem=send, recv_sem=recv,
            device_id=device, device_id_type=MESH,
        )
        sends.append(copy)
        return copy

    for j in range(ITERS):
        for l in order:
            y_ref[j, l] = m_ref[l] * v_ref[j, l]
        for side in range(2):
            at = pl.ds((0, rows - 1)[side], 1)
            for k in range(2):
                corner_out[j, 2 * k + side] = y_ref[j, ends[k], at, :]
            for l in range(layers):
                edge_out[j, 0, side, l] = y_ref[j, l, at, :]
        if j == 0:
            pl.semaphore_wait(barrier, greetings)
        edges = [
            [
                remote(
                    edge_out.at[j, part, side], edge_in.at[j, part, 1 - side],
                    edge_send.at[j, part, side], edge_recv.at[j, part, 1 - side],
                    (ix, y_of[side]),
                )
                for side in range(2)
            ]
            for part in range(2)
        ]
        relayed = near and j == 0
        corners = [
            remote(
                edge_in.at[j, 0, side, ends[k]] if relayed else corner_out.at[j, 2 * k + side],
                corner_in.at[j, 2 * (1 - k) + (side if relayed else 1 - side)],
                corner_send.at[j, 2 * k + side],
                corner_recv.at[j, 2 * (1 - k) + (side if relayed else 1 - side)],
                (x_of[k], iy if relayed else y_of[side]),
            )
            for k in range(2)
            for side in range(2)
        ]
        faces = [
            [
                remote(
                    src.at[j, ends[k]], face_ref.at[j, 1 - k, part],
                    face_send.at[j, k, part], face_recv.at[j, 1 - k, part],
                    (x_of[k], iy),
                )
                for k in range(2)
            ]
            for part, src in enumerate((y_ref, t_ref))
        ]
        for copy in edges[0] + ([] if relayed else corners) + faces[0]:
            copy.start()
        get_y = lambda l: y_ref[j, l]
        for l in order:
            t_ref[j, l] = local_k(get_y, l)
        for side in range(2):
            for l in range(layers):
                at = pl.ds((0, rows - 1)[side], 1)
                edge_out[j, 1, side, l] = t_ref[j, l, at, :]
        for copy in edges[1] + faces[1]:
            copy.start()
        mu.append(tile_sum(sum(v_ref[j, l] * y_ref[j, l] for l in range(layers))))
        for i in range(j + 1):
            dots[i, j] = tile_sum(sum(v_ref[i, l] * v_ref[j, l] for l in range(layers)))
        for copy in edges[0]:
            copy.wait_recv()
        if relayed:
            for copy in corners:
                copy.start()
        for copy in faces[0]:
            copy.wait_recv()
        full = ITERS + j % 2
        for l in range(layers):
            t = t_ref[j, l]
            if l == 0:
                t = t - face_ref[j, 0, 0]
            if l == layers - 1:
                t = t - face_ref[j, 1, 0]
            t_ref[full, l] = t
            for side in range(2):
                at = pl.ds((0, rows - 1)[side], 1)
                t_ref[full, l, at, :] = t_ref[full, l, at, :] - edge_in[j, 0, side, l]
        mu.append(tile_sum(sum(t_ref[full, l] * t_ref[full, l] for l in range(layers))))
        if j == ITERS - 1:
            start_sums(mu, dots, slots, sum_send, sum_recv, me, count, ny)
        get_t = lambda l: t_ref[full, l]
        for l in range(layers):
            v = local_k(get_t, l)
            for k in range(2):
                if l == ends[k]:
                    v = v + y_ref[j, l]
            v_ref[j + 1, l] = v
            for side in range(2):
                at = pl.ds((0, rows - 1)[side], 1)
                v_ref[j + 1, l, at, :] = v_ref[j + 1, l, at, :] + y_ref[j, l, at, :]
        for copy in edges[1] + corners:
            copy.wait_recv()
        for l in range(layers):
            for side in range(2):
                at = pl.ds((0, rows - 1)[side], 1)
                line = v_ref[j + 1, l, at, :] - edge_in[j, 1, side, l]
                for k in range(2):
                    if l == ends[k]:
                        line = line + 2.0 * corner_in[j, 2 * k + side]
                v_ref[j + 1, l, at, :] = line
        for copy in faces[1]:
            copy.wait_recv()
        for k in range(2):
            v_ref[j + 1, ends[k]] = v_ref[j + 1, ends[k]] - face_ref[j, k, 1]

    for copy in sends:
        copy.wait_send()
    all_slots = slots.at[pl.ds(0, count - 1)]
    pltpu.make_async_copy(all_slots, all_slots, sum_send).wait()
    pltpu.make_async_copy(all_slots, all_slots, sum_recv).wait()
    total = jnp.sum(slots[...], axis=0)
    names = [("mu", i) for i in range(2 * ITERS)] + sorted(dots)
    got = {name: total[:, k : k + 1] for k, name in enumerate(names)}
    mu = [got["mu", i] for i in range(2 * ITERS)]
    sol, res, norms = coefficients(mu, got, float(cells))
    for k, value in enumerate(norms + sol[:ITERS] + res[1:]):
        coef_ref[k] = value[0, 0]


def start_sums(mu, dots, slots, sum_send, sum_recv, me, count, ny):
    lane = lax.broadcasted_iota(jnp.int32, (1, slots.shape[-1]), 1)
    line = jnp.zeros(lane.shape, jnp.float32)
    for k, value in enumerate(mu + [dots[name] for name in sorted(dots)]):
        line = jnp.where(lane == k, value, line)
    slots[me] = line

    def send(k, carry):
        other = lax.rem(me + k, count)
        pltpu.make_async_remote_copy(
            src_ref=slots.at[me],
            dst_ref=slots.at[me],
            send_sem=sum_send,
            recv_sem=sum_recv,
            device_id=(other // ny, lax.rem(other, ny)),
            device_id_type=MESH,
        ).start()
        return carry

    lax.fori_loop(1, count, send, 0)


def finish(coef, v_ref, y_ref, sol_ref, res_ref, norms_ref):
    for i in range(ITERS):
        norms_ref[i] = coef[i]
    for l in range(v_ref.shape[1]):
        sol = coef[ITERS] * y_ref[0, l]
        res = v_ref[0, l]
        for i in range(1, ITERS):
            sol = sol + coef[ITERS + i] * y_ref[i, l]
        for i in range(1, ITERS + 1):
            res = res + coef[2 * ITERS + i - 1] * v_ref[i, l]
        sol_ref[l] = sol
        res_ref[l] = res


def body(right_side, kappa_sq):
    nx, ny = lax.axis_size("gx"), lax.axis_size("gy")
    shape = right_side.shape
    layers, rows, cols = shape
    cells = nx * layers * ny * rows * cols
    f32 = jnp.float32
    dma = pltpu.SemaphoreType.DMA
    whole = pl.BlockSpec(memory_space=pltpu.VMEM)
    smem = pl.BlockSpec(memory_space=pltpu.SMEM)
    out = pl.pallas_call(
        functools.partial(kernel, nx, ny, cells),
        out_shape=(
            pltpu.VMEM((ITERS + 1,) + shape, f32),
            pltpu.VMEM((ITERS,) + shape, f32),
            pltpu.SMEM((3 * ITERS,), f32),
        ),
        in_specs=[pl.BlockSpec(memory_space=pl.ANY)] * 2,
        out_specs=(whole, whole, smem),
        scratch_shapes=[
            pltpu.VMEM((ITERS + 2,) + shape, f32),
            pltpu.VMEM(shape, f32),
            pltpu.VMEM(shape, f32),
            pltpu.VMEM((ITERS, 2, 2, rows, cols), f32),
            pltpu.VMEM((ITERS, 2, 2, layers, 1, cols), f32),
            pltpu.VMEM((ITERS, 2, 2, layers, 1, cols), f32),
            pltpu.VMEM((ITERS, 4, 1, cols), f32),
            pltpu.VMEM((ITERS, 4, 1, cols), f32),
            pltpu.VMEM((nx * ny, 1, 128), f32),
            dma((2,)),
            dma((ITERS, 2, 2)),
            dma((ITERS, 2, 2)),
            dma((ITERS, 2, 2)),
            dma((ITERS, 2, 2)),
            dma((ITERS, 4)),
            dma((ITERS, 4)),
            dma(()),
            dma(()),
        ],
        compiler_params=pltpu.CompilerParams(collective_id=0, has_side_effects=True),
    )(right_side, kappa_sq)
    return pl.pallas_call(
        finish,
        out_shape=(
            jax.ShapeDtypeStruct(shape, f32),
            jax.ShapeDtypeStruct(shape, f32),
            jax.ShapeDtypeStruct((ITERS,), f32),
        ),
        in_specs=[smem, whole, whole],
        out_specs=(whole, whole, smem),
    )(out[2], *(pltpu.with_memory_space_constraint(x, pltpu.VMEM) for x in out[:2]))


def solution(mesh):
    return jax.shard_map(
        body,
        mesh=mesh,
        in_specs=(P("gx", "gy", None), P("gx", "gy", None)),
        out_specs=(P("gx", "gy", None), P("gx", "gy", None), P()),
        check_vma=False,
    )
```

```python
import functools
import jax
import jax.numpy as jnp
from jax import lax
from jax.experimental import pallas as pl
from jax.experimental.pallas import tpu as pltpu
from jax.sharding import PartitionSpec as P

ITERS = 3
MESH = pl.DeviceIdType.MESH


def shifted(c):
    return [None] + c[:-1]


def plus(a, b, scale):
    out = []
    for one, two in zip(a, b):
        two = None if two is None else two * scale
        out.append(one if two is None else two if one is None else one + two)
    return out


def form(c, entry):
    total = None
    for i, one in enumerate(c):
        for j, two in enumerate(c):
            if one is not None and two is not None and i < ITERS and j < ITERS:
                term = one * two * entry(i, j)
                total = term if total is None else total + term
    return total


def coefficients(mu, dots, cells):
    one = jnp.ones_like(mu[0])
    res = [one] + [None] * ITERS
    step = [None] * (ITERS + 1)
    sol = [None] * (ITERS + 1)
    norms = []
    for i in range(ITERS):
        gamma = form(res, lambda a, b: mu[a + b])
        delta = form(res, lambda a, b: mu[a + b + 1])
        norms.append(jnp.sqrt(form(res, lambda a, b: dots[min(a, b), max(a, b)]) / cells))
        if i == 0:
            alpha = gamma / delta
            step = list(res)
        else:
            beta = gamma / gamma_old
            alpha = gamma / (delta - beta * gamma / alpha_old)
            step = plus(res, step, beta)
        sol = plus(sol, step, alpha)
        res = plus(res, shifted(step), -alpha)
        gamma_old, alpha_old = gamma, alpha
    return sol, res, norms


def kernel(
    nx, ny, cells, rhs_hbm, kappa_hbm, *refs,
):
    (
    v_ref, y_ref, coef_ref, t_ref, d_ref, m_ref, face_ref, edge_out, edge_in, corner_out, corner_in,
    slots, load_sem, face_send, face_recv, edge_send, edge_recv, corner_send, corner_recv,
    sum_send, sum_recv,
    ) = refs
    layers, rows, cols = rhs_hbm.shape
    ix, iy = lax.axis_index("gx"), lax.axis_index("gy")
    count = nx * ny
    me = ix * ny + iy
    load_k = pltpu.make_async_copy(kappa_hbm, d_ref, load_sem.at[0])
    load_r = pltpu.make_async_copy(rhs_hbm, v_ref.at[0], load_sem.at[1])
    load_k.start()
    load_r.start()

    barrier = pltpu.get_barrier_semaphore()

    near = ny // 2 <= ITERS

    def greet(x, y):
        pl.semaphore_signal(barrier, inc=1, device_id=(x, y), device_id_type=MESH)

    def greet_any(k, carry):
        other = lax.rem(me + k, count)
        greet(other // ny, lax.rem(other, ny))
        return carry

    def greet_x(k, carry):
        greet(lax.rem(ix + k, nx), iy)
        return carry

    def greet_y(k, carry):
        greet(ix, lax.rem(iy + k, ny))
        return carry

    if near:
        lax.fori_loop(1, ny, greet_y, 0)
        lax.fori_loop(1, nx, greet_x, 0)
        greetings = nx - 1 + ny - 1
    else:
        lax.fori_loop(1, count, greet_any, 0)
        greetings = count - 1

    x_of = (lax.rem(ix + nx - 1, nx), lax.rem(ix + 1, nx))
    y_of = (lax.rem(iy + ny - 1, ny), lax.rem(iy + 1, ny))
    row = lax.broadcasted_iota(jnp.int32, (rows, cols), 0)
    first, last = row == 0, row == rows - 1

    def lateral(x):
        up = jnp.where(first, 0.0, pltpu.roll(x, 1, 0))
        down = jnp.where(last, 0.0, pltpu.roll(x, rows - 1, 0))
        return (pltpu.roll(x, 1, 1) + pltpu.roll(x, cols - 1, 1)) + (up + down)

    def local_k(get, l):
        x = get(l)
        out = d_ref[l] * x - lateral(x)
        if l > 0:
            out = out - get(l - 1)
        if l < layers - 1:
            out = out - get(l + 1)
        return out

    def tile_sum(x):
        return jnp.sum(x, axis=(0, 1), keepdims=True)

    load_k.wait()
    for l in range(layers):
        d = 6.0 + d_ref[l]
        d_ref[l] = d
        m_ref[l] = 1.0 / (d * d + 6.0)
    load_r.wait()

    ends = (0, layers - 1)
    mu, dots = ([], {})
    sends = []
    order = [0, layers - 1] + list(range(1, layers - 1)) if layers > 1 else [0]
    inner_first = list(range(1, layers - 1)) + [0, layers - 1] if layers > 1 else [0]

    def remote(src, dst, send, recv, device):
        copy = pltpu.make_async_remote_copy(
            src_ref=src, dst_ref=dst, send_sem=send, recv_sem=recv,
            device_id=device, device_id_type=MESH,
        )
        sends.append(copy)
        return copy

    for j in range(ITERS):
        for l in order:
            y_ref[j, l] = m_ref[l] * v_ref[j, l]
        for side in range(2):
            at = pl.ds((0, rows - 1)[side], 1)
            for k in range(2):
                corner_out[j, 2 * k + side] = y_ref[j, ends[k], at, :]
            for l in range(layers):
                edge_out[j, 0, side, l] = y_ref[j, l, at, :]
        if j == 0:
            pl.semaphore_wait(barrier, greetings)
        edges = [
            [
                remote(
                    edge_out.at[j, part, side], edge_in.at[j, part, 1 - side],
                    edge_send.at[j, part, side], edge_recv.at[j, part, 1 - side],
                    (ix, y_of[side]),
                )
                for side in range(2)
            ]
            for part in range(2)
        ]
        relayed = near and j == 0
        corners = [
            remote(
                edge_in.at[j, 0, side, ends[k]] if relayed else corner_out.at[j, 2 * k + side],
                corner_in.at[j, 2 * (1 - k) + (side if relayed else 1 - side)],
                corner_send.at[j, 2 * k + side],
                corner_recv.at[j, 2 * (1 - k) + (side if relayed else 1 - side)],
                (x_of[k], iy if relayed else y_of[side]),
            )
            for k in range(2)
            for side in range(2)
        ]
        faces = [
            [
                remote(
                    src.at[j, ends[k]], face_ref.at[j, 1 - k, part],
                    face_send.at[j, k, part], face_recv.at[j, 1 - k, part],
                    (x_of[k], iy),
                )
                for k in range(2)
            ]
            for part, src in enumerate((y_ref, t_ref))
        ]
        for copy in edges[0] + ([] if relayed else corners) + faces[0]:
            copy.start()
        get_y = lambda l: y_ref[j, l]
        for l in order:
            t_ref[j, l] = local_k(get_y, l)
        for side in range(2):
            for l in range(layers):
                at = pl.ds((0, rows - 1)[side], 1)
                edge_out[j, 1, side, l] = t_ref[j, l, at, :]
        for copy in edges[1] + faces[1]:
            copy.start()
        mu.append(tile_sum(sum(v_ref[j, l] * y_ref[j, l] for l in range(layers))))
        for i in range(j + 1):
            dots[i, j] = tile_sum(sum(v_ref[i, l] * v_ref[j, l] for l in range(layers)))
        for side in range(2):
            edges[0][1 - side].wait_recv()
            if relayed:
                corners[side].start()
                corners[2 + side].start()
        for copy in faces[0]:
            copy.wait_recv()
        full = ITERS + j % 2
        for l in range(layers):
            t = t_ref[j, l]
            if l == 0:
                t = t - face_ref[j, 0, 0]
            if l == layers - 1:
                t = t - face_ref[j, 1, 0]
            t_ref[full, l] = t
            for side in range(2):
                at = pl.ds((0, rows - 1)[side], 1)
                t_ref[full, l, at, :] = t_ref[full, l, at, :] - edge_in[j, 0, side, l]
        mu.append(tile_sum(sum(t_ref[full, l] * t_ref[full, l] for l in range(layers))))
        if j == ITERS - 1:
            start_sums(mu, dots, slots, sum_send, sum_recv, me, nx, ny)
        get_t = lambda l: t_ref[full, l]
        for l in range(layers):
            v = local_k(get_t, l)
            for k in range(2):
                if l == ends[k]:
                    v = v + y_ref[j, l]
            v_ref[j + 1, l] = v
            for side in range(2):
                at = pl.ds((0, rows - 1)[side], 1)
                v_ref[j + 1, l, at, :] = v_ref[j + 1, l, at, :] + y_ref[j, l, at, :]
        for copy in edges[1] + corners:
            copy.wait_recv()
        for l in range(layers):
            for side in range(2):
                at = pl.ds((0, rows - 1)[side], 1)
                line = v_ref[j + 1, l, at, :] - edge_in[j, 1, side, l]
                for k in range(2):
                    if l == ends[k]:
                        line = line + 2.0 * corner_in[j, 2 * k + side]
                v_ref[j + 1, l, at, :] = line
        for copy in faces[1]:
            copy.wait_recv()
        for k in range(2):
            v_ref[j + 1, ends[k]] = v_ref[j + 1, ends[k]] - face_ref[j, k, 1]

    for copy in sends:
        copy.wait_send()
    all_slots = slots.at[pl.ds(0, count - 1)]
    pltpu.make_async_copy(all_slots, all_slots, sum_send).wait()
    pltpu.make_async_copy(all_slots, all_slots, sum_recv).wait()
    total = jnp.sum(slots[...], axis=0)
    names = [("mu", i) for i in range(2 * ITERS)] + sorted(dots)
    got = {
        name: jnp.broadcast_to(total[:, k : k + 1], total.shape) for k, name in enumerate(names)
    }
    mu = [got["mu", i] for i in range(2 * ITERS)]
    sol, res, norms = coefficients(mu, got, float(cells))
    for k, value in enumerate(norms + sol[:ITERS] + res[1:]):
        coef_ref[k] = value[0, 0]


def start_sums(mu, dots, slots, sum_send, sum_recv, me, nx, ny):
    lane = lax.broadcasted_iota(jnp.int32, (1, slots.shape[-1]), 1)
    line = jnp.zeros(lane.shape, jnp.float32)
    for k, value in enumerate(mu + [dots[name] for name in sorted(dots)]):
        line = jnp.where(lane == k, value, line)
    slots[me] = line

    def send(x, y):
        pltpu.make_async_remote_copy(
            src_ref=slots.at[me],
            dst_ref=slots.at[me],
            send_sem=sum_send,
            recv_sem=sum_recv,
            device_id=(x, y),
            device_id_type=MESH,
        ).start()

    ix, iy = lax.axis_index("gx"), lax.axis_index("gy")
    y_at = [lax.rem(iy + k, ny) for k in range(ny)]

    def send_line(k, carry):
        x = ix + k
        x = jnp.where(x >= nx, x - nx, x)
        for y in y_at[1:] + y_at[:1]:
            send(x, y)
        return carry

    lax.fori_loop(1, nx, send_line, 0)
    for y in y_at[1:]:
        send(ix, y)


def finish(coef, v_ref, y_ref, sol_ref, res_ref, norms_ref):
    for i in range(ITERS):
        norms_ref[i] = coef[i]
    for l in range(v_ref.shape[1]):
        sol = coef[ITERS] * y_ref[0, l]
        res = v_ref[0, l]
        for i in range(1, ITERS):
            sol = sol + coef[ITERS + i] * y_ref[i, l]
        for i in range(1, ITERS + 1):
            res = res + coef[2 * ITERS + i - 1] * v_ref[i, l]
        sol_ref[l] = sol
        res_ref[l] = res


def body(right_side, kappa_sq):
    nx, ny = lax.axis_size("gx"), lax.axis_size("gy")
    shape = right_side.shape
    layers, rows, cols = shape
    cells = nx * layers * ny * rows * cols
    f32 = jnp.float32
    dma = pltpu.SemaphoreType.DMA
    whole = pl.BlockSpec(memory_space=pltpu.VMEM)
    smem = pl.BlockSpec(memory_space=pltpu.SMEM)
    out = pl.pallas_call(
        functools.partial(kernel, nx, ny, cells),
        out_shape=(
            pltpu.VMEM((ITERS + 1,) + shape, f32),
            pltpu.VMEM((ITERS,) + shape, f32),
            pltpu.SMEM((3 * ITERS,), f32),
        ),
        in_specs=[pl.BlockSpec(memory_space=pl.ANY)] * 2,
        out_specs=(whole, whole, smem),
        scratch_shapes=[
            pltpu.VMEM((ITERS + 2,) + shape, f32),
            pltpu.VMEM(shape, f32),
            pltpu.VMEM(shape, f32),
            pltpu.VMEM((ITERS, 2, 2, rows, cols), f32),
            pltpu.VMEM((ITERS, 2, 2, layers, 1, cols), f32),
            pltpu.VMEM((ITERS, 2, 2, layers, 1, cols), f32),
            pltpu.VMEM((ITERS, 4, 1, cols), f32),
            pltpu.VMEM((ITERS, 4, 1, cols), f32),
            pltpu.VMEM((nx * ny, 1, 128), f32),
            dma((2,)),
            dma((ITERS, 2, 2)),
            dma((ITERS, 2, 2)),
            dma((ITERS, 2, 2)),
            dma((ITERS, 2, 2)),
            dma((ITERS, 4)),
            dma((ITERS, 4)),
            dma(()),
            dma(()),
        ],
        compiler_params=pltpu.CompilerParams(collective_id=0, has_side_effects=True),
    )(right_side, kappa_sq)
    return pl.pallas_call(
        finish,
        out_shape=(
            jax.ShapeDtypeStruct(shape, f32),
            jax.ShapeDtypeStruct(shape, f32),
            jax.ShapeDtypeStruct((ITERS,), f32),
        ),
        in_specs=[smem, whole, whole],
        out_specs=(whole, whole, smem),
    )(out[2], *(pltpu.with_memory_space_constraint(x, pltpu.VMEM) for x in out[:2]))


def solution(mesh):
    return jax.shard_map(
        body,
        mesh=mesh,
        in_specs=(P("gx", "gy", None), P("gx", "gy", None)),
        out_specs=(P("gx", "gy", None), P("gx", "gy", None), P()),
        check_vma=False,
    )
```
